256 devices in a mesh: py: 8 (over z_lo, core), px: 4 (over y), pz: 2 (over z_hi), site: 4 (over x).
Axes of the slice: x: 4, y: 4, z: 8 (z_hi: 2, z_lo: 4; z = z_hi * 4 + z_lo), core: 2. Of those that a mesh axis runs over, the one named last changes fastest.
Arguments:
- density: float32 [1024, 16, 128, 128], P(('site', 'py'), 'px', 'pz'), parts along dimension 0, may hold values from 0.2 to 1.8
- diffusivity: float32 [1024, 16, 128, 128], P(('site', 'py'), 'px', 'pz'), parts along dimension 0, may hold values from 0.03 to 0.15
- source: float32 [1024, 16, 128, 128], P(('site', 'py'), 'px', 'pz'), parts along dimension 0, may hold values from -0.2 to 0.2
Outputs:
- density_end: float32 [1024, 16, 128, 128], P(('site', 'py'), 'px', 'pz'), parts along dimension 0
The draws below stay inside these ranges and needn't reach their ends.
There are 4 independent parts, one for each index of `site`. The reference program is written for one: setup_inputs(seed, part) draws one part's arguments, and reference() takes and returns one part's arrays. A program takes and returns all parts, laid end to end along the dimension named above; each array names one. Nothing has to cross between parts.
All inputs are finite; a program needn't handle non-finite values.
Results may differ from the reference program's by a relative error of at most 0.00002.
Values sent between devices are 32-bit elements; how exact they have to be, the bound alone decides.
No kernel may reach another device: no remote copies, remote signals or barrier semaphores. Data moves between devices by JAX's collectives and lax.ppermute only.
A program may use at most 192 MiB of HBM per device.

```python
import jax
import jax.numpy as jnp
from jax import lax

GRID_J = 256
GRID_I = 16
GRID_K = 128
MEMBERS = 128
STEPS = 4


def level_of(own_key, shape, split, smallest, largest):
    level, own = 1.0, jax.random.fold_in(own_key, 6)
    for axis_at, parts in split:
        heights = jnp.exp(jax.random.uniform(jax.random.fold_in(own, axis_at), (parts,), jnp.float32, smallest / len(split), largest / len(split)))
        level = level * jnp.repeat(heights, shape[axis_at] // parts).reshape([-1 if axis == axis_at else 1 for axis in range(len(shape))])
    return level


def setup_inputs(seed: int = 0, part: int = 0) -> dict:
    streams_of = jax.random.split(jax.random.key(seed), 4)
    part_splits = jax.random.split(jax.random.fold_in(streams_of[3], part), 4)
    density = jnp.clip(0.2 + 1.5999999 * jax.random.uniform(part_splits[0], (GRID_J, GRID_I, GRID_K, MEMBERS), jnp.float32) ** level_of(part_splits[0], (GRID_J, GRID_I, GRID_K, MEMBERS), ((0, 8), (1, 4), (2, 2)), -0.2, 0.2), 0.2, 1.8)
    diffusivity = jnp.clip(0.03 + 0.120000007 * jax.random.uniform(part_splits[1], (GRID_J, GRID_I, GRID_K, MEMBERS), jnp.float32) ** level_of(part_splits[1], (GRID_J, GRID_I, GRID_K, MEMBERS), ((0, 8), (1, 4), (2, 2)), -0.2, 0.2), 0.03, 0.15)
    source = jnp.clip(jax.random.uniform(part_splits[2], (GRID_J, GRID_I, GRID_K, MEMBERS), jnp.float32, -0.2, 0.2) * level_of(part_splits[2], (GRID_J, GRID_I, GRID_K, MEMBERS), ((0, 8), (1, 4), (2, 2)), -0.4, 0.0), -0.2, 0.2)
    return {"density": density, "diffusivity": diffusivity, "source": source}


def inner_cells(values, dims):
    for dim in dims:
        values = lax.slice_in_dim(values, 1, values.shape[dim] - 1, axis=dim)
    return values


def side_cells(values, dim, start, dims):
    others = [other for other in dims if other != dim]
    values = inner_cells(values, others)
    return lax.slice_in_dim(values, start, start + values.shape[dim] - 2, axis=dim)


def advance(padded, diffusivity, source):
    middle = inner_cells(padded, (0, 1, 2))
    lower = [side_cells(padded, dim, 0, (0, 1, 2)) for dim in (0, 1, 2)]
    upper = [side_cells(padded, dim, 2, (0, 1, 2)) for dim in (0, 1, 2)]
    spread = lower[0] + upper[0] + lower[1] + upper[1] + lower[2] + upper[2] - 6.0 * middle
    return middle + diffusivity * spread + source


def reference(density, diffusivity, source):
    for step in range(STEPS):
        density = advance(jnp.pad(density, ((1, 1), (1, 1), (1, 1), (0, 0)), mode="constant"), diffusivity, source)
    return density
```

```python
import functools

import jax
import jax.numpy as jnp
from jax import lax
from jax.experimental import pallas as pl
from jax.experimental.pallas import tpu as pltpu
from jax.sharding import PartitionSpec as P

STEPS = 4
CUTS = (0, 16, 32)
VMEM, HBM = pltpu.VMEM, pltpu.HBM


def call(kernel, outs, args, flops=0, moved=0, **extra):
    return pl.pallas_call(
        kernel,
        out_shape=outs,
        compiler_params=pltpu.CompilerParams(vmem_limit_bytes=4 * 2**20),
        cost_estimate=pl.CostEstimate(flops=flops, bytes_accessed=moved, transcendentals=0),
        **extra,
    )(*args)


def in_vmem(n):
    return [pl.BlockSpec(memory_space=VMEM)] * n


def faces_kernel(start, stop, u_ref, low_ref, high_ref, sems):
    rows = pl.ds(start, stop - start)
    last = u_ref.shape[1] - 1
    a = pltpu.make_async_copy(u_ref.at[rows, 0], low_ref, sems.at[0])
    b = pltpu.make_async_copy(u_ref.at[rows, last], high_ref, sems.at[1])
    a.start()
    b.start()
    a.wait()
    b.wait()


def faces(u, start, stop):
    shape = (stop - start,) + u.shape[2:]
    out = VMEM(shape, u.dtype)
    return call(
        functools.partial(faces_kernel, start, stop),
        (out, out),
        (pltpu.with_memory_space_constraint(u, HBM),),
        flops=10**7,
        moved=4 * shape[0] * shape[1] * shape[2],
        in_specs=[pl.BlockSpec(memory_space=HBM)],
        out_specs=tuple(in_vmem(2)),
        scratch_shapes=[pltpu.SemaphoreType.DMA((2,))],
    )


def edges_kernel(cuts, u_ref, low_ref, high_ref, *edge_refs):
    total, width, depth = u_ref.shape[:3]
    mine = jnp.where(lax.axis_index("pz") == 0, depth - 1, 0)
    for start, stop, edge_ref in zip(cuts[:-1], cuts[1:], edge_refs):

        def row(j, carry):
            for i in range(width):
                edge_ref[pl.ds((j - start) * width + i, 1), :] = u_ref[j, i, pl.ds(mine, 1), :]
            return carry

        lax.fori_loop(start, stop, row, 0)
    for i in range(width):
        low_ref[0, i] = u_ref[0, i]
        high_ref[0, i] = u_ref[total - 1, i]


def edges(u, cuts):
    _, width, depth, lanes = u.shape
    outs = [VMEM((1,) + u.shape[1:], u.dtype)] * 2
    outs += [VMEM(((b - a) * width, lanes), u.dtype) for a, b in zip(cuts[:-1], cuts[1:])]
    return call(
        functools.partial(edges_kernel, cuts),
        tuple(outs),
        (u,),
        flops=10**6,
        moved=4 * u.size // depth,
        in_specs=in_vmem(1),
        out_specs=tuple(in_vmem(len(outs))),
    )


def step_kernel(start, rows, own, before, after, final, *refs):
    u_ref, before_ref, after_ref, low_ref, high_ref, edge_ref, d_ref, s_ref = refs[:8]
    width, depth = u_ref.shape[1], u_ref.shape[2]
    place = lax.axis_index("pz")
    mine = jnp.where(place == 0, depth - 1, 0)
    if final is None:
        new_ref, to_low, to_high, to_edge = refs[8:12]
        to_end = refs[12] if len(refs) > 12 else None
    else:
        out_ref, new_ref, sem = refs[-3:]

    def send(j):
        pltpu.make_async_copy(new_ref.at[j], out_ref.at[start + j], sem).start()

    def advance(j, below, above):
        for i in range(width):
            middle = u_ref[own + j, i]
            side_low = low_ref[j] if i == 0 else u_ref[own + j, i - 1]
            side_high = high_ref[j] if i == width - 1 else u_ref[own + j, i + 1]
            edge = edge_ref[pl.ds(j * width + i, 1), :]
            k_low = jnp.where(place == 0, 0.0, edge)
            k_high = jnp.where(place == 0, edge, 0.0)
            k_lower = jnp.concatenate([k_low, middle[:-1]], axis=0)
            k_upper = jnp.concatenate([middle[1:], k_high], axis=0)
            spread = below(i) + above(i) + side_low + side_high + k_lower + k_upper - 6.0 * middle
            value = middle + d_ref[start + j, i] * spread + s_ref[start + j, i]
            new_ref[j, i] = value
            if final is None:
                if i == 0:
                    to_low[j] = value
                if i == width - 1:
                    to_high[j] = value
                to_edge[pl.ds(j * width + i, 1), :] = new_ref[j, i, pl.ds(mine, 1), :]

    advance(0, lambda i: before_ref[before, i], lambda i: u_ref[own + 1, i])

    def loop(j, carry):
        advance(j, lambda i: u_ref[own + j - 1, i], lambda i: u_ref[own + j + 1, i])
        if final is not None:
            send(j - 1)
        return carry

    lax.fori_loop(1, rows - 1, loop, 0)
    advance(rows - 1, lambda i: u_ref[own + rows - 2, i], lambda i: after_ref[after, i])
    if final is not None:
        send(rows - 2)
        send(rows - 1)
        pltpu.make_async_copy(new_ref, out_ref.at[pl.ds(start, rows)], sem).wait()
    elif to_end is not None:
        end = 0 if start == 0 else rows - 1
        for i in range(width):
            to_end[0, i] = new_ref[end, i]


def step(start, rows, u, before, after, halo, fields, whole=None, final=False, total=None):
    (u, own), (before, before_at), (after, after_at) = u, before, after
    _, width, depth, lanes = u.shape
    args = [u, before, after, *halo, *fields]
    specs = in_vmem(8)
    extra = {}
    if final:
        outs = jax.ShapeDtypeStruct((total, width, depth, lanes), u.dtype)
        out_specs = pl.BlockSpec(memory_space=HBM)
        extra["scratch_shapes"] = [VMEM((rows, width, depth, lanes), u.dtype), pltpu.SemaphoreType.DMA]
        if whole is not None:
            args.append(whole)
            specs.append(pl.BlockSpec(memory_space=HBM))
            extra["input_output_aliases"] = {8: 0}
    else:
        outs = [VMEM((rows, width, depth, lanes), u.dtype)]
        outs += [VMEM((rows, depth, lanes), u.dtype)] * 2
        outs += [VMEM((rows * width, lanes), u.dtype)]
        if start == 0 or start + rows == total:
            outs += [VMEM((1, width, depth, lanes), u.dtype)]
        outs, out_specs = tuple(outs), tuple(in_vmem(len(outs)))
    size = rows * width * depth * lanes
    return call(
        functools.partial(step_kernel, start, rows, own, before_at, after_at, final or None),
        outs,
        args,
        flops=12 * size,
        moved=4 * size,
        in_specs=specs,
        out_specs=out_specs,
        **extra,
    )


def shift(x, axis, to_next):
    pairs = [(i, i + 1) for i in range(lax.axis_size(axis) - 1)]
    if not to_next:
        pairs = [(b, a) for a, b in pairs]
    return lax.ppermute(x, axis, pairs)


def swap(x):
    return lax.ppermute(x, "pz", [(0, 1), (1, 0)])


def body(density, diffusivity, source):
    total = density.shape[0]
    parts = list(zip(CUTS[:-1], CUTS[1:]))
    n = len(parts)
    low, high, edge = [None] * n, [None] * n, [None] * n
    fields = (diffusivity, source)
    for c, (a, b) in enumerate(parts):
        to_low, to_high = faces(density, a, b)
        low[c] = shift(to_high, "px", True)
        high[c] = shift(to_low, "px", False)
    first, last, *ends = edges(density, CUTS)
    above = shift(first, "py", False)
    below = shift(last, "py", True)
    for c in range(n):
        edge[c] = swap(ends[c])
    u = [(density, a) for a, b in parts]
    whole = None
    for t in range(STEPS):
        final = t == STEPS - 1
        old, old_below, old_above = list(u), below, above
        for c, (a, b) in enumerate(parts):
            before = (old_below, 0) if c == 0 else (old[c - 1][0], old[c - 1][1] + a - parts[c - 1][0] - 1)
            after = (old_above, 0) if c == n - 1 else old[c + 1]
            out = step(a, b - a, old[c], before, after, (low[c], high[c], edge[c]), fields, whole, final, total)
            if final:
                whole = out
                continue
            u[c] = (out[0], 0)
            low[c] = shift(out[2], "px", True)
            high[c] = shift(out[1], "px", False)
            edge[c] = swap(out[3])
            if c == 0:
                above = shift(out[4], "py", False)
            if c == n - 1:
                below = shift(out[4], "py", True)
    return whole


def solution(mesh):
    placed = P(("site", "py"), "px", "pz", None)
    return jax.shard_map(body, mesh=mesh, in_specs=(placed,) * 3, out_specs=placed, check_vma=False)
```

```python
import functools

import jax
import jax.numpy as jnp
from jax import lax
from jax.experimental import pallas as pl
from jax.experimental.pallas import tpu as pltpu
from jax.sharding import PartitionSpec as P

STEPS = 4
CUTS = (0, 16, 32)
VMEM, HBM = pltpu.VMEM, pltpu.HBM


def in_vmem(n):
    return [pl.BlockSpec(memory_space=VMEM)] * n


def call(kernel, outs, args, flops, moved, **extra):
    return pl.pallas_call(
        kernel,
        out_shape=outs,
        compiler_params=pltpu.CompilerParams(vmem_limit_bytes=4 * 2**20),
        cost_estimate=pl.CostEstimate(flops=flops, bytes_accessed=moved, transcendentals=0),
        **extra,
    )(*args)


def exchange(x, axis, round_):
    size = lax.axis_size(axis)
    pairs = [p for i in range(round_, size - 1, 2) for p in ((i, i + 1), (i + 1, i))]
    return lax.ppermute(x, axis, pairs)


def is_even(axis):
    return lax.rem(lax.axis_index(axis), 2) == 0


def toward(axis, last):
    even = is_even(axis)
    return jnp.where(even, last, 0), jnp.where(even, 0, last)


def faces_kernel(start, rows, u_ref, one_ref, two_ref, sems):
    one, two = toward("px", u_ref.shape[1] - 1)
    a = pltpu.make_async_copy(u_ref.at[pl.ds(start, rows), one], one_ref, sems.at[0])
    b = pltpu.make_async_copy(u_ref.at[pl.ds(start, rows), two], two_ref, sems.at[1])
    a.start()
    b.start()
    a.wait()
    b.wait()


def faces(u, start, rows):
    shape = (rows,) + u.shape[2:]
    return call(
        functools.partial(faces_kernel, start, rows),
        (VMEM(shape, u.dtype),) * 2,
        (pltpu.with_memory_space_constraint(u, HBM),),
        10**7,
        2 * rows * u.size // u.shape[0],
        in_specs=[pl.BlockSpec(memory_space=HBM)],
        out_specs=tuple(in_vmem(2)),
        scratch_shapes=[pltpu.SemaphoreType.DMA((2,))],
    )


def edges_kernel(cuts, u_ref, one_ref, two_ref, *edge_refs):
    total, width, depth = u_ref.shape[:3]
    mine = jnp.where(lax.axis_index("pz") == 0, depth - 1, 0)
    one, two = toward("py", total - 1)
    for i in range(width):
        one_ref[0, i] = u_ref[one, i]
        two_ref[0, i] = u_ref[two, i]
    for start, stop, edge_ref in zip(cuts[:-1], cuts[1:], edge_refs):

        def row(j, carry):
            for i in range(width):
                edge_ref[pl.ds((j - start) * width + i, 1), :] = u_ref[j, i, pl.ds(mine, 1), :]
            return carry

        lax.fori_loop(start, stop, row, 0)


def edges(u, cuts):
    _, width, depth, lanes = u.shape
    outs = [VMEM((1,) + u.shape[1:], u.dtype)] * 2
    outs += [VMEM(((b - a) * width, lanes), u.dtype) for a, b in zip(cuts[:-1], cuts[1:])]
    return call(
        functools.partial(edges_kernel, cuts),
        tuple(outs),
        (u,),
        10**6,
        4 * u.size // depth,
        in_specs=in_vmem(1),
        out_specs=tuple(in_vmem(len(outs))),
    )


def step_kernel(start, rows, own, lower, upper, final, ends, *refs):
    u_ref, d_ref, s_ref, one_ref, two_ref, edge_ref = refs[:6]
    rest = list(refs[6:])
    lower_ref = rest.pop(0) if lower is not None else None
    upper_ref = rest.pop(0) if upper is not None else None
    halo_refs = (rest.pop(0), rest.pop(0)) if lower is None or upper is None else None
    head_ref = rest.pop(0) if ends else None
    width, depth = u_ref.shape[1], u_ref.shape[2]
    place = lax.axis_index("pz")
    mine = jnp.where(place == 0, depth - 1, 0)
    even, even_row = is_even("px"), is_even("py")
    one_at, two_at = toward("px", width - 1)
    if final:
        out_ref, new_ref, sem = rest[-3:]
    else:
        new_ref, to_one, to_two, to_edge = rest[:4]

    def send(j):
        pltpu.make_async_copy(new_ref.at[j], out_ref.at[start + j], sem).start()

    def advance(j, below, above):
        for i in range(width):
            middle = u_ref[own + j, i]
            side_low = jnp.where(even, two_ref[j], one_ref[j]) if i == 0 else u_ref[own + j, i - 1]
            side_high = jnp.where(even, one_ref[j], two_ref[j]) if i == width - 1 else u_ref[own + j, i + 1]
            edge = edge_ref[pl.ds(j * width + i, 1), :]
            k_lower = jnp.concatenate([jnp.where(place == 0, 0.0, edge), middle[:-1]], axis=0)
            k_upper = jnp.concatenate([middle[1:], jnp.where(place == 0, edge, 0.0)], axis=0)
            spread = below(i) + above(i) + side_low + side_high + k_lower + k_upper - 6.0 * middle
            new_ref[j, i] = middle + d_ref[start + j, i] * spread + s_ref[start + j, i]
            if not final:
                to_edge[pl.ds(j * width + i, 1), :] = new_ref[j, i, pl.ds(mine, 1), :]
        if not final:
            to_one[j] = new_ref[j, one_at]
            to_two[j] = new_ref[j, two_at]

    def below_first(i):
        if lower is not None:
            return lower_ref[lower, i]
        return jnp.where(even_row, halo_refs[1][0, i], halo_refs[0][0, i])

    def above_last(i):
        if upper is not None:
            return upper_ref[upper, i]
        return jnp.where(even_row, halo_refs[0][0, i], halo_refs[1][0, i])

    advance(0, below_first, lambda i: u_ref[own + 1, i])

    def loop(j, carry):
        advance(j, lambda i: u_ref[own + j - 1, i], lambda i: u_ref[own + j + 1, i])
        if final:
            send(j - 1)
        return carry

    lax.fori_loop(1, rows - 1, loop, 0)
    advance(rows - 1, lambda i: u_ref[own + rows - 2, i], above_last)
    if final:
        send(rows - 2)
        send(rows - 1)
        pltpu.make_async_copy(new_ref, out_ref.at[pl.ds(start, rows)], sem).wait()
    elif ends:
        for i in range(width):
            first, last = head_ref[0, i], new_ref[rows - 1, i]
            rest[4][0, i] = jnp.where(even_row, last, first)
            rest[5][0, i] = jnp.where(even_row, first, last)


def step(start, rows, u, lower, upper, fields, sides, halos, head, whole, final):
    total = fields[0].shape[0]
    _, width, depth, lanes = u[0].shape
    ends = not final and start + rows == total
    args = [u[0], *fields, *sides]
    args += [x[0] for x in (lower, upper) if x is not None]
    if lower is None or upper is None:
        args += halos
    if ends:
        args.append(head)
    specs = in_vmem(len(args))
    extra = {}
    if final:
        outs = jax.ShapeDtypeStruct(fields[0].shape, u[0].dtype)
        out_specs = pl.BlockSpec(memory_space=HBM)
        extra["scratch_shapes"] = [VMEM((rows, width, depth, lanes), u[0].dtype), pltpu.SemaphoreType.DMA]
        if whole is not None:
            extra["input_output_aliases"] = {len(args): 0}
            args.append(whole)
            specs.append(pl.BlockSpec(memory_space=HBM))
    else:
        shapes = [(rows, width, depth, lanes), (rows, depth, lanes), (rows, depth, lanes), (rows * width, lanes)]
        shapes += [(1, width, depth, lanes)] * (2 * ends)
        outs = tuple(VMEM(shape, u[0].dtype) for shape in shapes)
        out_specs = tuple(in_vmem(len(outs)))
    size = rows * width * depth * lanes
    at = [None if x is None else x[1] for x in (lower, upper)]
    return call(
        functools.partial(step_kernel, start, rows, u[1], *at, final, ends),
        outs,
        args,
        12 * size,
        4 * size,
        in_specs=specs,
        out_specs=out_specs,
        **extra,
    )


def body(density, diffusivity, source):
    parts = list(zip(CUTS[:-1], CUTS[1:]))
    n = len(parts)
    fields = [diffusivity, source]
    sides = [None] * n

    def swap(x):
        return lax.ppermute(x, "pz", [(0, 1), (1, 0)])

    def trade(one, two, edge):
        return [exchange(one, "px", 0), exchange(two, "px", 1), swap(edge)]

    outward = [faces(density, a, b - a) for a, b in parts]
    one, two, *ends = edges(density, CUTS)
    sides = [trade(*outward[c], ends[c]) for c in range(n)]
    halos = [exchange(one, "py", 0), exchange(two, "py", 1)]
    u = [(density, a) for a, _ in parts]
    whole = None
    for t in range(1, STEPS + 1):
        old, final = list(u), t == STEPS
        for c, (a, b) in enumerate(parts):
            lower = None if c == 0 else (old[c - 1][0], old[c - 1][1] + a - parts[c - 1][0] - 1)
            upper = None if c == n - 1 else old[c + 1]
            out = step(a, b - a, old[c], lower, upper, fields, sides[c], halos, u[0][0], whole, final)
            if final:
                whole = out
                continue
            u[c] = (out[0], 0)
            sides[c] = trade(*out[1:4])
        if not final:
            halos = [exchange(out[4], "py", 0), exchange(out[5], "py", 1)]
    return whole


def solution(mesh):
    placed = P(("site", "py"), "px", "pz", None)
    return jax.shard_map(body, mesh=mesh, in_specs=(placed,) * 3, out_specs=placed, check_vma=False)
```
